32 devices in a mesh: atom: 8 (over z, x), energy: 4 (over y, core).
Axes of the slice: x: 2, y: 2, z: 4, core: 2. Of those that a mesh axis runs over, the one named last changes fastest.
Arguments:
- t_matrix: float32 [4, 64, 16, 16], P('energy', 'atom'), may hold values from -1.5 to 1.5
- structure: bfloat16 [4, 64, 1024, 1024], P('energy', 'atom'), may hold values from -0.125 to 0.125
- radial: bfloat16 [4, 64, 16, 1024], P('energy', 'atom'), may hold values from -3 to 3
- weights: float32 [4], P('energy'), may hold values from 0.1 to 1
- neighbours: int32 [64, 64], P('atom'), may hold values from 0 to 63, as said below
- live: int32 [64, 64], P('atom'), may hold values from 0 to 1, as said below
Outputs:
- density: float32 [64, 1024], P('atom', 'energy')
The draws below stay inside these ranges and needn't reach their ends.
Inputs may be any that keep to these rules, and one draw needn't show every extreme that they name: `neighbours`: slot 0 of atom i holds i itself. Atom i lies at index i // 8 of the atom axis, and every neighbour of it lies at an index that differs from that one by at most 3 around the axis, which closes into a loop; both extremes occur in every draw. An atom may appear in several slots of one zone. `live`: each row is 1 on its first slots and 0 after; slot 0 is always 1, at least 16 slots are 1, and some atom has all 64 slots 1.
All inputs are finite; a program needn't handle non-finite values.
Results may differ from the reference program's by a relative error of at most 0.0043.
Values sent between devices are 32-bit elements; how exact they have to be, the bound alone decides.
No kernel may reach another device: no remote copies, remote signals or barrier semaphores. Data moves between devices by JAX's collectives and lax.ppermute only.
A program may use at most 128 MiB of HBM per device.

```python
import math
import jax
import jax.numpy as jnp
from jax import lax

LM = 16
NB = 64
R = 1024
ITERS = 4
SPAN = 3
A_DEV = 8
ATOMS = 64
ENERGIES = 4


def draw_neighbours(key, part):
    first_key, second_key = jax.random.split(jax.random.fold_in(key, 11))
    n_devices = ATOMS // A_DEV
    owner = jnp.arange(ATOMS, dtype=jnp.int32) // A_DEV
    offsets = jax.random.randint(first_key, (ATOMS, NB), -SPAN, SPAN + 1)
    offsets = offsets.at[:, 1].set(SPAN).at[:, 2].set(-SPAN)
    slots = jax.random.randint(second_key, (ATOMS, NB), 0, A_DEV)
    device = (owner[:, None] + offsets + n_devices) % n_devices
    picked = device * A_DEV + slots
    picked = picked.at[:, 0].set(jnp.arange(ATOMS, dtype=jnp.int32))
    return picked.astype(jnp.int32)


def draw_live(key, part):
    counts = jax.random.randint(jax.random.fold_in(key, 23), (ATOMS,), NB // 4, NB + 1)
    counts = counts.at[0].set(NB)
    return (jnp.arange(NB)[None, :] < counts[:, None]).astype(jnp.int32)


def block_levels(rng, shape, pieces, smallest, top_value):
    gain, own = 1.0, jax.random.fold_in(rng, 6)
    for axis_at, blocks in pieces:
        draws = jnp.exp(jax.random.uniform(jax.random.fold_in(own, axis_at), (blocks,), jnp.float32, smallest / len(pieces), top_value / len(pieces)))
        gain = gain * jnp.repeat(draws, shape[axis_at] // blocks).reshape([-1 if axis == axis_at else 1 for axis in range(len(shape))])
    return gain


def bell_draw(key, shape, deviation, most, cuts=(), kind=jnp.bfloat16):
    loudness = block_levels(key, shape, cuts, -0.22, 0.18) if cuts else 1.0
    drawn = jax.random.normal(key, shape, jnp.float32) * deviation * loudness
    return jnp.minimum(jnp.maximum(drawn, -most), most).astype(kind)


def setup_inputs(seed: int = 0) -> dict:
    splits = jax.random.split(jax.random.key(seed), 7)
    return {
        "t_matrix": bell_draw(splits[0], (ENERGIES, ATOMS, LM, LM), LM ** -0.5, 1.5, ((0, 4), (1, 8)), jnp.float32),
        "structure": bell_draw(splits[1], (ENERGIES, ATOMS, NB * LM, NB * LM), (2 * NB * LM) ** -0.5, 0.125, ((0, 4), (1, 8))),
        "radial": bell_draw(splits[2], (ENERGIES, ATOMS, LM, R), 0.5, 3.0, ((0, 4), (1, 8))),
        "weights": jnp.clip(jnp.exp(math.log(1.0) - 2.3025851 * jax.random.uniform(splits[3], (ENERGIES,), jnp.float32) ** block_levels(splits[3], (ENERGIES,), ((0, 4),), -0.2, 0.2)), 0.1, 1.0),
        "neighbours": draw_neighbours(jax.random.fold_in(splits[6], 71), 0),
        "live": draw_live(jax.random.fold_in(splits[6], 71), 0),
    }


def zone_column(args):
    t_self, g_here, zt_here = args
    rest = jnp.zeros((NB - 1, LM, LM), jnp.float32)
    first = jnp.concatenate([t_self[None], rest], axis=0)
    g_float = g_here.astype(jnp.float32)
    zt_float = zt_here.astype(jnp.float32)
    column = first
    for step in range(ITERS):
        flat_b = lax.optimization_barrier(column.astype(jnp.bfloat16))
        flat = flat_b.astype(jnp.float32).reshape(NB * LM, LM)
        image = jnp.dot(g_float, flat, precision=lax.Precision.HIGHEST)
        image_b = lax.optimization_barrier(image.astype(jnp.bfloat16))
        image_f = image_b.astype(jnp.float32).reshape(NB, LM, LM)
        column = first + jnp.einsum("sij,sjk->sik", zt_float, image_f, precision=lax.Precision.HIGHEST)
    return column


def reference(t_matrix, structure, radial, weights, neighbours, live):
    live_f = live.astype(jnp.float32)
    flat_ids = neighbours.reshape(-1)

    def per_energy(args):
        t_here, g_here, z_here = args
        zone_t = (t_here[neighbours] * live_f[:, :, None, None]).astype(jnp.bfloat16)
        column = lax.map(zone_column, (t_here, g_here, zone_t))
        blocks = (column * live_f[:, :, None, None]).reshape(ATOMS * NB, LM, LM)
        received = jax.ops.segment_sum(blocks, flat_ids, num_segments=ATOMS)
        received_b = lax.optimization_barrier(received.astype(jnp.bfloat16))
        z_float = z_here.astype(jnp.float32)
        turned = jnp.einsum("alm,amr->alr", received_b.astype(jnp.float32), z_float, precision=lax.Precision.HIGHEST)
        return jnp.sum(z_float * turned, axis=1)

    partial_value = lax.map(per_energy, (t_matrix, structure, radial))
    return jnp.sum(weights[:, None, None] * partial_value, axis=0)
```

```python
import functools

import jax
import jax.numpy as jnp
from jax import lax
from jax.experimental import pallas as pl
from jax.experimental.pallas import tpu as pltpu
from jax.sharding import PartitionSpec as P

ITERS = 4
SPAN = 3
TILE = 256
N_ACC = 4


def shifted(value, axis, by):
    devices = lax.axis_size(axis)
    return lax.ppermute(value, axis, [(i, (i + by) % devices) for i in range(devices)])


def dot_nt(a, b):
    return lax.dot_general(a, b, (((1,), (1,)), ((), ())), preferred_element_type=jnp.float32)


def zone_kernel(dims, idx_ref, first_ref, g_hbm, *refs):
    a_dev, zone, lm, places = dims
    t_refs = refs[:places]
    out_ref = refs[places]
    g, tab, bd, mask, img, colb, fin = refs[places + 1 : places + 8]
    accs = refs[places + 8 : places + 8 + N_ACC]
    sems = refs[places + 8 + N_ACC]
    width = zone * lm
    n_q = width // TILE
    per = TILE // lm
    rows = a_dev * lm

    def copy(a):
        return pltpu.make_async_copy(g_hbm.at[a], g.at[a], sems.at[a])

    for a in range(a_dev):
        copy(a).start()
    for acc in accs:
        acc[...] = jnp.zeros(acc.shape, jnp.float32)
    row_i = lax.broadcasted_iota(jnp.int32, (TILE, TILE), 0)
    col_i = lax.broadcasted_iota(jnp.int32, (TILE, TILE), 1)
    mask[...] = jnp.where(row_i // lm == col_i // lm, 1.0, 0.0).astype(jnp.bfloat16)
    rep_r = lax.broadcasted_iota(jnp.int32, (lm, TILE), 0)
    rep_c = lax.broadcasted_iota(jnp.int32, (lm, TILE), 1)
    rep = jnp.where(rep_r == rep_c % lm, 1.0, 0.0).astype(jnp.bfloat16)
    for p in range(places):
        piece = t_refs[p][...].reshape(rows, lm).astype(jnp.bfloat16)
        wide = jnp.dot(piece, rep, preferred_element_type=jnp.float32)
        tab[p * rows : (p + 1) * rows, :] = wide.astype(jnp.bfloat16)
    tab[places * rows : places * rows + lm, :] = jnp.zeros((lm, TILE), jnp.bfloat16)

    def build(a, carry):
        for s in range(zone):
            at = pl.multiple_of(idx_ref[a, s] * lm, lm)
            m = s % per
            bd[a, s * lm : (s + 1) * lm, :] = tab[pl.ds(at, lm), :] * mask[m * lm : (m + 1) * lm, :]
        return carry

    lax.fori_loop(0, a_dev, build, 0)

    for a in range(a_dev):
        copy(a).wait()
        img[a] = dot_nt(first_ref[a].astype(jnp.bfloat16), g[a, :, :TILE]).astype(jnp.bfloat16)

    def sweep(step, carry):
        for a in range(a_dev):
            for q in range(n_q):
                cut = slice(q * TILE, (q + 1) * TILE)
                c = dot_nt(img[a, :, cut], bd[a, cut, :])
                if q == 0:
                    c = c + first_ref[a]
                colb[a, :, cut] = c.astype(jnp.bfloat16)
        for a in range(a_dev):
            img[a] = dot_nt(colb[a], g[a]).astype(jnp.bfloat16)
        return carry

    lax.fori_loop(0, ITERS - 1, sweep, 0)

    for a in range(a_dev):
        for q in range(n_q):
            cut = slice(q * TILE, (q + 1) * TILE)
            f = dot_nt(bd[a, cut, :], img[a, :, cut])
            fin[a, cut, :] = f
        fin[a, :lm, :] = fin[a, :lm, :] + t_refs[SPAN][a]

    def scatter(a, carry):
        for s in range(zone):
            at = pl.multiple_of(idx_ref[a, s] * lm, lm)
            acc = accs[s % N_ACC]
            acc[pl.ds(at, lm), :] = acc[pl.ds(at, lm), :] + fin[a, s * lm : (s + 1) * lm, :]
        return carry

    lax.fori_loop(0, a_dev, scatter, 0)

    for p in range(places):
        total = accs[0][p * rows : (p + 1) * rows, :]
        for acc in accs[1:]:
            total = total + acc[p * rows : (p + 1) * rows, :]
        out_ref[p] = jnp.concatenate([total[a * lm : (a + 1) * lm] for a in range(a_dev)], axis=1)


def density_kernel(dims, me_ref, w_ref, *refs):
    a_dev, lm, places, parts = dims
    pieces = refs[:places]
    radial_ref = refs[places]
    outs = refs[places + 1 : places + 1 + parts]
    buf = refs[places + 1 + parts]
    total = pieces[0][...]
    for piece in pieces[1:]:
        total = total + piece[...]
    rows = a_dev * lm
    tall = jnp.concatenate([total] * a_dev, axis=0)
    row_i = lax.broadcasted_iota(jnp.int32, (rows, rows), 0)
    col_i = lax.broadcasted_iota(jnp.int32, (rows, rows), 1)
    block = jnp.where(row_i // lm == col_i // lm, tall, 0.0).astype(jnp.bfloat16)
    radial = radial_ref[...].reshape(rows, -1)
    turned = jnp.dot(block, radial, preferred_element_type=jnp.float32)
    prod = turned * radial.astype(jnp.float32)
    buf[...] = w_ref[0] * jnp.sum(prod.reshape(a_dev, lm, -1), axis=1)
    cut = buf.shape[1] // parts
    for d in range(parts):
        at = pl.multiple_of(((me_ref[0] + d) % parts) * cut, cut)
        outs[d][...] = buf[:, pl.ds(at, cut)]


def shards(t_matrix, structure, radial, weights, neighbours, live):
    a_dev, lm = t_matrix.shape[1], t_matrix.shape[2]
    zone = neighbours.shape[1]
    n_r = radial.shape[3]
    n_atom = lax.axis_size("atom")
    n_energy = lax.axis_size("energy")
    me = lax.axis_index("atom")
    places = 2 * SPAN + 1
    width = zone * lm
    rows = a_dev * lm
    t_own = t_matrix[0]
    pieces = [t_own] * places
    for place in range(places):
        if place != SPAN:
            pieces[place] = shifted(t_own, "atom", SPAN - place)
    place_of = (neighbours // a_dev - me + SPAN + n_atom) % n_atom
    target = place_of * a_dev + neighbours % a_dev
    index = jnp.where(live != 0, target, a_dev * places)
    first = jnp.pad(jnp.swapaxes(t_own, 1, 2), ((0, 0), (0, 0), (0, TILE - lm)))

    smem = pl.BlockSpec(memory_space=pltpu.SMEM)
    vmem = pl.BlockSpec(memory_space=pltpu.VMEM)
    acc_shape = pltpu.VMEM(((places * a_dev + 1) * lm, lm), jnp.float32)
    sent = pl.pallas_call(
        functools.partial(zone_kernel, (a_dev, zone, lm, places)),
        name="zone",
        out_shape=jax.ShapeDtypeStruct((places, lm, rows), jnp.float32),
        in_specs=[smem, vmem, pl.BlockSpec(memory_space=pl.ANY)] + [vmem] * places,
        out_specs=vmem,
        scratch_shapes=[
            pltpu.VMEM((a_dev, width, width), jnp.bfloat16),
            pltpu.VMEM(((places * a_dev + 1) * lm, TILE), jnp.bfloat16),
            pltpu.VMEM((a_dev, width, TILE), jnp.bfloat16),
            pltpu.VMEM((TILE, TILE), jnp.bfloat16),
            pltpu.VMEM((a_dev, lm, width), jnp.bfloat16),
            pltpu.VMEM((a_dev, lm, width), jnp.bfloat16),
            pltpu.VMEM((a_dev, width, lm), jnp.float32),
        ]
        + [acc_shape] * N_ACC
        + [pltpu.SemaphoreType.DMA((a_dev,))],
        compiler_params=pltpu.CompilerParams(vmem_limit_bytes=48 * 1024 * 1024),
    )(index, first, structure[0], *pieces)

    got = [sent[SPAN]]
    for place in range(places):
        if place != SPAN:
            got.append(shifted(sent[place], "atom", place - SPAN))
    cut = n_r // n_energy
    mine = lax.axis_index("energy").astype(jnp.int32).reshape(1)
    chunks = pl.pallas_call(
        functools.partial(density_kernel, (a_dev, lm, places, n_energy)),
        name="density",
        out_shape=[jax.ShapeDtypeStruct((a_dev, cut), jnp.float32)] * n_energy,
        in_specs=[smem, smem] + [vmem] * (places + 1),
        out_specs=[vmem] * n_energy,
        scratch_shapes=[pltpu.VMEM((a_dev, n_r), jnp.float32)],
    )(mine, weights, *got, radial[0])
    total = chunks[0]
    for d in range(1, n_energy):
        total = total + shifted(chunks[d], "energy", d)
    return total


def solution(mesh):
    in_specs = (
        P("energy", "atom", None, None),
        P("energy", "atom", None, None),
        P("energy", "atom", None, None),
        P("energy"),
        P("atom", None),
        P("atom", None),
    )
    out_specs = P("atom", "energy")
    return jax.shard_map(shards, mesh=mesh, in_specs=in_specs, out_specs=out_specs, check_vma=False)
```

```python
import functools

import jax
import jax.numpy as jnp
from jax import lax
from jax.experimental import pallas as pl
from jax.experimental.pallas import tpu as pltpu
from jax.sharding import PartitionSpec as P

ITERS = 4
SPAN = 3
TILE = 256
N_ACC = 4


def shifted(value, axis, by):
    devices = lax.axis_size(axis)
    return lax.ppermute(value, axis, [(i, (i + by) % devices) for i in range(devices)])


def dot_nt(a, b):
    return lax.dot_general(a, b, (((1,), (1,)), ((), ())), preferred_element_type=jnp.float32)


def zone_kernel(dims, idx_ref, first_ref, g_hbm, *refs):
    a_dev, zone, lm, places = dims
    t_refs = refs[:places]
    out_ref = refs[places]
    g, tab, bd, mask, img, colb, fin = refs[places + 1 : places + 8]
    accs = refs[places + 8 : places + 8 + N_ACC]
    sems = refs[places + 8 + N_ACC]
    width = zone * lm
    n_q = width // TILE
    per = TILE // lm
    rows = a_dev * lm

    def copy(a):
        return pltpu.make_async_copy(g_hbm.at[a], g.at[a], sems.at[a])

    for a in range(a_dev):
        copy(a).start()
    for acc in accs:
        acc[...] = jnp.zeros(acc.shape, jnp.float32)
    row_i = lax.broadcasted_iota(jnp.int32, (TILE, TILE), 0)
    col_i = lax.broadcasted_iota(jnp.int32, (TILE, TILE), 1)
    mask[...] = jnp.where(row_i // lm == col_i // lm, 1.0, 0.0).astype(jnp.bfloat16)
    rep_r = lax.broadcasted_iota(jnp.int32, (lm, TILE), 0)
    rep_c = lax.broadcasted_iota(jnp.int32, (lm, TILE), 1)
    rep = jnp.where(rep_r == rep_c % lm, 1.0, 0.0).astype(jnp.bfloat16)
    for p in range(places):
        piece = t_refs[p][...].reshape(rows, lm).astype(jnp.bfloat16)
        wide = jnp.dot(piece, rep, preferred_element_type=jnp.float32)
        tab[p * rows : (p + 1) * rows, :] = wide.astype(jnp.bfloat16)
    tab[places * rows : places * rows + lm, :] = jnp.zeros((lm, TILE), jnp.bfloat16)

    def build(a, carry):
        for s in range(zone):
            at = pl.multiple_of(idx_ref[a, s] * lm, lm)
            m = s % per
            bd[a, s * lm : (s + 1) * lm, :] = tab[pl.ds(at, lm), :] * mask[m * lm : (m + 1) * lm, :]
        return carry

    lax.fori_loop(0, a_dev, build, 0)

    for a in range(a_dev):
        copy(a).wait()
        img[a] = dot_nt(first_ref[a].astype(jnp.bfloat16), g[a, :, :TILE]).astype(jnp.bfloat16)

    def sweep(step, carry):
        for a in range(a_dev):
            for q in range(n_q):
                cut = slice(q * TILE, (q + 1) * TILE)
                c = dot_nt(img[a, :, cut], bd[a, cut, :])
                if q == 0:
                    c = c + first_ref[a]
                colb[a, :, cut] = c.astype(jnp.bfloat16)
        for a in range(a_dev):
            img[a] = dot_nt(colb[a], g[a]).astype(jnp.bfloat16)
        return carry

    lax.fori_loop(0, ITERS - 1, sweep, 0)

    for a in range(a_dev):
        for q in range(n_q):
            cut = slice(q * TILE, (q + 1) * TILE)
            f = dot_nt(bd[a, cut, :], img[a, :, cut])
            fin[a, cut, :] = f
        fin[a, :lm, :] = fin[a, :lm, :] + t_refs[SPAN][a]

    def scatter(a, carry):
        for s in range(zone):
            at = pl.multiple_of(idx_ref[a, s] * lm, lm)
            acc = accs[s % N_ACC]
            acc[pl.ds(at, lm), :] = acc[pl.ds(at, lm), :] + fin[a, s * lm : (s + 1) * lm, :]
        return carry

    lax.fori_loop(0, a_dev, scatter, 0)

    for p in range(places):
        total = accs[0][p * rows : (p + 1) * rows, :]
        for acc in accs[1:]:
            total = total + acc[p * rows : (p + 1) * rows, :]
        out_ref[p] = jnp.concatenate([total[a * lm : (a + 1) * lm] for a in range(a_dev)], axis=1)


def density_kernel(dims, me_ref, w_ref, *refs):
    a_dev, lm, places, parts = dims
    pieces = refs[:places]
    radial_ref = refs[places]
    outs = refs[places + 1 : places + 1 + parts]
    buf = refs[places + 1 + parts]
    total = pieces[0][...]
    for piece in pieces[1:]:
        total = total + piece[...]
    rows = a_dev * lm
    tall = jnp.concatenate([total] * a_dev, axis=0)
    row_i = lax.broadcasted_iota(jnp.int32, (rows, rows), 0)
    col_i = lax.broadcasted_iota(jnp.int32, (rows, rows), 1)
    block = jnp.where(row_i // lm == col_i // lm, tall, 0.0).astype(jnp.bfloat16)
    radial = radial_ref[...].reshape(rows, -1)
    turned = jnp.dot(block, radial, preferred_element_type=jnp.float32)
    prod = turned * radial.astype(jnp.float32)
    buf[...] = w_ref[0] * jnp.sum(prod.reshape(a_dev, lm, -1), axis=1)
    cut = buf.shape[1] // parts
    for d in range(parts):
        at = pl.multiple_of(((me_ref[0] + d) % parts) * cut, cut)
        outs[d][...] = buf[:, pl.ds(at, cut)]


def shards(t_matrix, structure, radial, weights, neighbours, live):
    a_dev, lm = t_matrix.shape[1], t_matrix.shape[2]
    zone = neighbours.shape[1]
    n_r = radial.shape[3]
    n_atom = lax.axis_size("atom")
    n_energy = lax.axis_size("energy")
    me = lax.axis_index("atom")
    places = 2 * SPAN + 1
    width = zone * lm
    rows = a_dev * lm
    t_own = t_matrix[0]
    pieces = [t_own] * places
    for place in range(places):
        if place != SPAN:
            pieces[place] = shifted(t_own, "atom", SPAN - place)
    place_of = (neighbours // a_dev - me + SPAN + n_atom) % n_atom
    target = place_of * a_dev + neighbours % a_dev
    index = jnp.where(live != 0, target, a_dev * places)
    first = jnp.pad(jnp.swapaxes(t_own, 1, 2), ((0, 0), (0, 0), (0, TILE - lm)))

    smem = pl.BlockSpec(memory_space=pltpu.SMEM)
    vmem = pl.BlockSpec(memory_space=pltpu.VMEM)
    acc_shape = pltpu.VMEM(((places * a_dev + 1) * lm, lm), jnp.float32)
    sent = pl.pallas_call(
        functools.partial(zone_kernel, (a_dev, zone, lm, places)),
        name="zone",
        out_shape=jax.ShapeDtypeStruct((places, lm, rows), jnp.float32),
        in_specs=[smem, vmem, pl.BlockSpec(memory_space=pl.ANY)] + [vmem] * places,
        out_specs=vmem,
        scratch_shapes=[
            pltpu.VMEM((a_dev, width, width), jnp.bfloat16),
            pltpu.VMEM(((places * a_dev + 1) * lm, TILE), jnp.bfloat16),
            pltpu.VMEM((a_dev, width, TILE), jnp.bfloat16),
            pltpu.VMEM((TILE, TILE), jnp.bfloat16),
            pltpu.VMEM((a_dev, lm, width), jnp.bfloat16),
            pltpu.VMEM((a_dev, lm, width), jnp.bfloat16),
            pltpu.VMEM((a_dev, width, lm), jnp.float32),
        ]
        + [acc_shape] * N_ACC
        + [pltpu.SemaphoreType.DMA((a_dev,))],
        compiler_params=pltpu.CompilerParams(vmem_limit_bytes=48 * 1024 * 1024),
    )(index, first, structure[0], *pieces)

    got = [sent[SPAN]]
    for place in range(places):
        if place != SPAN:
            got.append(shifted(sent[place], "atom", place - SPAN))
    cut = n_r // n_energy
    mine = lax.axis_index("energy").astype(jnp.int32).reshape(1)
    chunks = pl.pallas_call(
        functools.partial(density_kernel, (a_dev, lm, places, n_energy)),
        name="density",
        out_shape=[jax.ShapeDtypeStruct((a_dev, cut), jnp.float32)] * n_energy,
        in_specs=[smem, smem] + [vmem] * (places + 1),
        out_specs=[vmem] * n_energy,
        scratch_shapes=[pltpu.VMEM((a_dev, n_r), jnp.float32)],
        compiler_params=pltpu.CompilerParams(vmem_limit_bytes=8 * 1024 * 1024),
    )(mine, weights, *got, radial[0])
    total = chunks[0]
    for d in range(1, n_energy):
        total = total + shifted(chunks[d], "energy", d)
    return total


def solution(mesh):
    in_specs = (
        P("energy", "atom", None, None),
        P("energy", "atom", None, None),
        P("energy", "atom", None, None),
        P("energy"),
        P("atom", None),
        P("atom", None),
    )
    out_specs = P("atom", "energy")
    return jax.shard_map(shards, mesh=mesh, in_specs=in_specs, out_specs=out_specs, check_vma=False)
```
